256 devices in a mesh: vox: 128 (over x, z, y), sub: 2 (over core).
Axes of the slice: x: 4, y: 4, z: 8, core: 2. Of those that a mesh axis runs over, the one named last changes fastest.
Arguments:
- movie: bfloat16 [262144, 4096], P(('vox', 'sub')), may hold values from -120 to 120
- test_matrix: bfloat16 [4096, 256], replicated, may hold values from -0.09375 to 0.09375
Outputs:
- basis: float32 [262144, 256], P(('vox', 'sub'))
- r_factor: float32 [256, 256], replicated
- projected: float32 [256, 4096], P(None, ('vox', 'sub'))
The draws below stay inside these ranges and needn't reach their ends.
All inputs are finite; a program needn't handle non-finite values.
Results may differ from the reference program's by a relative error of at most 0.00063.
Values sent between devices are 32-bit elements; how exact they have to be, the bound alone decides.
A program may use at most 128 MiB of HBM per device.

```python
import jax
import jax.numpy as jnp
from jax import lax

FRAMES = 4096
RANK = 256
VOXELS = 262144


def draw_movie(key, part):
    key_base = jax.random.fold_in(key, 11)
    key_scale = jax.random.fold_in(key, 12)
    row_index = jnp.arange(VOXELS, dtype=jnp.float32)
    rising = 1.0 + 2.0 * row_index / VOXELS
    spread = jnp.exp(jax.random.uniform(key_scale, (VOXELS,), jnp.float32) * jnp.log(10.0))
    row_scale = (rising * spread)[:, None]
    base = jax.random.normal(key_base, (VOXELS, FRAMES), jnp.float32)
    base = jnp.clip(base, -4.0, 4.0)
    return (base * row_scale).astype(jnp.bfloat16)


def noise(rng, shape, scale, most, kind=jnp.bfloat16):
    drawn = jax.random.normal(rng, shape, jnp.float32) * scale
    return jnp.minimum(jnp.maximum(drawn, -most), most).astype(kind)


def setup_inputs(seed: int = 0) -> dict:
    splits = jax.random.split(jax.random.key(seed), 3)
    movie = draw_movie(jax.random.fold_in(splits[2], 71), 0)
    test_matrix = noise(splits[1], (FRAMES, RANK), FRAMES ** -0.5, 0.09375)
    return dict(movie=movie, test_matrix=test_matrix)


def reference(movie, test_matrix):
    sketch = jnp.dot(movie.astype(jnp.float32), test_matrix.astype(jnp.float32), preferred_element_type=jnp.float32)
    gram = jnp.dot(sketch.T, sketch, precision=lax.Precision.HIGHEST)
    lower = jnp.linalg.cholesky(gram)
    identity = jnp.eye(RANK, dtype=jnp.float32)
    inverse = lax.linalg.triangular_solve(lower, identity, left_side=True, lower=True)
    scale = jnp.sqrt(jnp.float32(VOXELS))
    basis = jnp.dot(sketch, inverse.T, precision=lax.Precision.HIGHEST) * scale
    sketch_b = sketch.astype(jnp.bfloat16)
    cross = lax.dot_general(sketch_b.astype(jnp.float32), movie.astype(jnp.float32), (((0,), (0,)), ((), ())), preferred_element_type=jnp.float32)
    projected = jnp.dot(inverse, cross, precision=lax.Precision.HIGHEST)
    return (basis, lower.T / scale, projected)
```

```python
import jax
import jax.numpy as jnp
from jax import lax
from jax.experimental import pallas as pl
from jax.experimental.pallas import tpu as pltpu
from jax.sharding import PartitionSpec as P

F = jnp.float32
HI = lax.Precision.HIGHEST
MESH = pl.DeviceIdType.MESH
VMEM = pltpu.VMEM
DMA = pltpu.SemaphoreType.DMA
NX, NZ, NY = 4, 8, 4
CHUNKS, WIDE = 8, 512


def place(x, z, y, s):
    return ((x * NZ + z) * NY + y, s)


def remote(src, dst, send, recv, device):
    return pltpu.make_async_remote_copy(
        src_ref=src, dst_ref=dst, send_sem=send, recv_sem=recv, device_id=device, device_id_type=MESH
    )


def each(lo, hi, body):
    lax.fori_loop(lo, hi, lambda i, c: (body(i), c)[1], 0)


def factor64(block, left):
    lane = lax.broadcasted_iota(jnp.int32, (8, 128), 1)
    sub = lax.broadcasted_iota(jnp.int32, (8, 128), 0)
    here = (lane < 64) if left else (lane >= 64)
    at, eye = (0, 64) if left else (64, 0)
    rows = [jnp.where(here, block[8 * v:8 * v + 8, :], (lane == eye + 8 * v + sub).astype(F)) for v in range(8)]
    pivots = []
    for p in range(8):
        first = at + 8 * p
        cols = [[jnp.broadcast_to(rows[v][:, first + j:first + j + 1], (8, 128)) for v in range(p, 8)] for j in range(8)]
        pivot = jnp.ones((8, 128), F)
        for k in range(8):
            d = jnp.broadcast_to(cols[k][0][k:k + 1, :], (8, 128))
            pivot = jnp.where(sub == k, d, pivot)
            r = 1.0 / d
            m = [c * r for c in cols[k]]
            m[0] = jnp.where(sub > k, m[0], 0.0)
            row = jnp.broadcast_to(rows[p][k:k + 1, :], (8, 128))
            for j in range(k + 1, 8):
                u = jnp.broadcast_to(cols[j][0][k:k + 1, :], (8, 128))
                cols[j] = [c - a * u for c, a in zip(cols[j], m)]
            for v in range(p, 8):
                rows[v] = rows[v] - m[v - p] * row
        pivots.append(pivot)
    out = [lax.rsqrt(d) * r for d, r in zip(pivots, rows)]
    keep = [jnp.where(here & (lane - at < 8 * v + sub), 0.0, out[v]) for v in range(8)]
    return jnp.concatenate(keep, axis=0)


def factor256(t_ref, diag_ref):
    col = lax.broadcasted_iota(jnp.int32, (64, 256), 1)
    row64 = lax.broadcasted_iota(jnp.int32, (64, 256), 0)
    for s in range(4):
        r0 = 64 * s
        tile = 128 * (s // 2)
        left = s % 2 == 0
        t = t_ref[r0:r0 + 64, :]
        both = factor64(t[:, tile:tile + 128], left)
        diag_ref[r0:r0 + 64, :] = both
        y = jnp.where((col >= r0) & (col < r0 + 64), (col - r0 == row64).astype(F), t)
        z = jnp.zeros((64, 256), F)
        us = jnp.dot(both, jnp.concatenate([z, y] if left else [y, z], axis=0), precision=HI, preferred_element_type=F)
        t_ref[r0:r0 + 64, :] = us
        if s < 3:
            full = lax.dot_general(us, us, (((0,), (0,)), ((), ())), precision=HI, preferred_element_type=F)
            colr = lax.broadcasted_iota(jnp.int32, (192 - r0, 256), 1)
            rest = t_ref[r0 + 64:, :]
            t_ref[r0 + 64:, :] = jnp.where((colr >= r0) & (colr < r0 + 64), 0.0, rest) - full[r0 + 64:, :]


def parts(t_ref, diag_ref):
    col = lax.broadcasted_iota(jnp.int32, (256, 256), 1)
    row = lax.broadcasted_iota(jnp.int32, (256, 256), 0)
    t = t_ref[...]
    d = diag_ref[...]
    dd = jnp.concatenate([d, d], axis=1)
    upper = jnp.where(col // 64 == row // 64, dd, t)
    return jnp.where(col >= row, upper, 0.0), jnp.where(col <= row, t, 0.0)


def reduce_kernel(
    movie, test, sketch, gram, cross,
    mv, tv, skt, skb, part, drecv, half, gpart, grs, gz, a_tmp, a_in, b_tmp, b_in, pa, pb, r2, p2, r3,
    msem, tsem, dsend, drsem, gs_send, gs_recv, gz_send, gz_recv, ga_send, ga_recv,
    s1_send, s1_recv, s2_send, s2_recv, s3_send, s3_recv, s4_send, s4_recv,
):
    vox, s = lax.axis_index("vox"), lax.axis_index("sub")
    y = lax.rem(vox, NY)
    z = lax.rem(lax.div(vox, NY), NZ)
    x = lax.div(vox, NY * NZ)
    q = (x * NY + y) * 2 + s
    other = place(x, z, y, 1 - s)

    def load(c):
        wide = pl.ds(pl.multiple_of(c * WIDE, WIDE), WIDE)
        return (
            pltpu.make_async_copy(movie.at[:, wide], mv.at[c], msem.at[c]),
            pltpu.make_async_copy(test.at[wide], tv.at[c], tsem.at[c]),
        )

    def start(c):
        for copy in load(c):
            copy.start()

    each(0, CHUNKS, start)

    def plane(d):
        t = lax.rem(q + d, 32)
        return t, place(lax.div(t, NY * 2), z, lax.rem(lax.div(t, 2), NY), lax.rem(t, 2))

    def column(d):
        t = lax.rem(z + d, NZ)
        return t, place(x, t, y, s)

    barrier = pltpu.get_barrier_semaphore()

    def greet(device):
        pl.semaphore_signal(barrier, inc=1, device_id=device, device_id_type=MESH)

    each(1, 32, lambda d: greet(plane(d)[1]))
    each(1, NZ, lambda d: greet(column(d)[1]))

    sketch[...] = jnp.zeros_like(sketch)

    def project(c):
        for copy in load(c):
            copy.wait()
        sketch[...] += jnp.dot(mv[c], tv[c], preferred_element_type=F)

    each(0, CHUNKS, project)
    skt[...] = jnp.transpose(sketch[...])
    skb[...] = skt[...].astype(jnp.bfloat16)
    gpart[...] = jnp.dot(skt[...], sketch[...], precision=HI, preferred_element_type=F).reshape(32, 8, 256)

    pl.semaphore_wait(barrier, 31 + NZ - 1)

    def gram_scatter(d):
        t, device = plane(d)
        return remote(gpart.at[t], grs.at[d], gs_send.at[d], gs_recv.at[d], device)

    each(1, 32, lambda d: gram_scatter(d).start())

    def across(c):
        rows = pl.ds(pl.multiple_of((1 - s) * 128, 128), 128)
        return remote(part.at[c, rows], drecv.at[c], dsend.at[c], drsem.at[c], other)

    def multiply(c):
        part[c] = jnp.dot(skb[...], mv[c], preferred_element_type=F)
        across(c).start()

    each(0, CHUNKS, multiply)

    each(1, 32, lambda d: gram_scatter(d).wait_recv())
    total = gpart[q]
    for d in range(1, 32):
        total = total + grs[d]
    gz[z] = total

    def gram_column(d):
        t, device = column(d)
        return remote(gz.at[z], gz.at[z], gz_send.at[d], gz_recv.at[d], device)

    def gram_column_from(d):
        t = lax.rem(z - d + NZ, NZ)
        return remote(gz.at[t], gz.at[t], gz_send.at[d], gz_recv.at[d], place(x, t, y, s))

    each(1, NZ, lambda d: gram_column(d).start())

    def fold(c):
        across(c).wait_recv()
        half[c] = part[c, pl.ds(pl.multiple_of(s * 128, 128), 128)] + drecv[c]

    each(0, CHUNKS, fold)

    xr, xo, xl = (lax.rem(x + d, NX) for d in (1, 2, 3))
    yr, yo, yl = (lax.rem(y + d, NY) for d in (1, 2, 3))
    right_x, left_x = place(xr, z, y, s), place(xl, z, y, s)
    right_y, left_y = place(x, z, yr, s), place(x, z, yl, s)

    def rows(i):
        return pl.ds(pl.multiple_of(i * 32, 32), 32)

    def ring(i, src, dst, device):
        return remote(src, dst, s1_send.at[i], s1_recv.at[i], device)

    ring_a = [
        ring(0, half.at[2 * xo], a_tmp.at[0], right_x),
        ring(1, half.at[2 * xo + 1], a_tmp.at[1], left_x),
        ring(2, half.at[2 * xr + 1], a_in.at[0, 1], right_x),
        ring(3, half.at[2 * xl], a_in.at[1, 0], left_x),
        ring(4, half.at[2 * xr], a_in.at[0, 0], right_x),
        ring(5, half.at[2 * xl + 1], a_in.at[1, 1], left_x),
    ]
    lo, hi = pl.ds(0, 4), pl.ds(4, 4)
    ring_b = [
        ring(0, half.at[lo, rows(yo)], b_tmp.at[0], right_y),
        ring(1, half.at[hi, rows(yo)], b_tmp.at[1], left_y),
        ring(2, half.at[hi, rows(yr)], b_in.at[0, hi], right_y),
        ring(3, half.at[lo, rows(yl)], b_in.at[1, lo], left_y),
        ring(4, half.at[lo, rows(yr)], b_in.at[0, lo], right_y),
        ring(5, half.at[hi, rows(yl)], b_in.at[1, hi], left_y),
    ]

    @pl.when(s == 0)
    def _():
        for copy in ring_a[:4]:
            copy.start()

    @pl.when(s == 1)
    def _():
        for copy in ring_b[:4]:
            copy.start()

    each(1, NZ, lambda d: gram_column_from(d).wait_recv())
    each(1, NZ, lambda d: gram_column(d).wait_send())
    total = gz[0]
    for j in range(1, NZ):
        total = total + gz[j]
    gram[q] = total

    def gram_gather(d):
        t, device = plane(d)
        return remote(gram.at[q], gram.at[q], ga_send.at[d], ga_recv.at[d], device)

    def gram_gather_from(d):
        t, device = plane(32 - d)
        return remote(gram.at[t], gram.at[t], ga_send.at[d], ga_recv.at[d], device)

    each(1, 32, lambda d: gram_gather(d).start())

    @pl.when(s == 0)
    def _():
        ring_a[0].wait_recv()
        half[2 * xr] = half[2 * xr] + a_tmp[0]
        ring_a[4].start()
        ring_a[1].wait_recv()
        half[2 * xl + 1] = half[2 * xl + 1] + a_tmp[1]
        ring_a[5].start()
        for copy in ring_a[2:]:
            copy.wait_recv()
        pa[...] = half[pl.ds(2 * x, 2)] + a_in[0] + a_in[1]

    @pl.when(s == 1)
    def _():
        ring_b[0].wait_recv()
        half[lo, rows(yr)] = half[lo, rows(yr)] + b_tmp[0]
        ring_b[4].start()
        ring_b[1].wait_recv()
        half[hi, rows(yl)] = half[hi, rows(yl)] + b_tmp[1]
        ring_b[5].start()
        for copy in ring_b[2:]:
            copy.wait_recv()
        pb[...] = half[:, rows(y)] + b_in[0] + b_in[1]

    def second_a(d):
        t = (yr, yo, yl)[d]
        return remote(pa.at[:, rows(t)], r2.at[d], s2_send.at[d], s2_recv.at[d], place(x, z, t, s))

    def second_b(d):
        t = (xr, xo, xl)[d]
        return remote(pb.at[pl.ds(2 * t, 2)], r2.at[d], s2_send.at[d], s2_recv.at[d], place(t, z, y, s))

    @pl.when(s == 0)
    def _():
        for d in range(3):
            second_a(d).start()
        for d in range(3):
            second_a(d).wait_recv()
        p2[...] = pa[:, rows(y)] + r2[0] + r2[1] + r2[2]

    @pl.when(s == 1)
    def _():
        for d in range(3):
            second_b(d).start()
        for d in range(3):
            second_b(d).wait_recv()
        p2[...] = pb[pl.ds(2 * x, 2)] + r2[0] + r2[1] + r2[2]

    def tile(t):
        return lax.div(t, 4), slice(None), pl.ds(pl.multiple_of(lax.rem(t, 4) * 128, 128), 128)

    def third(d):
        t, device = column(d)
        return remote(p2.at[tile(t)], r3.at[d], s3_send.at[d], s3_recv.at[d], device)

    each(1, NZ, lambda d: third(d).start())
    each(1, NZ, lambda d: third(d).wait_recv())
    total = p2[tile(z)]
    for d in range(1, NZ):
        total = total + r3[d]
    cross[rows(s * 4 + y)] = total

    def fourth(d):
        t = lax.rem(s * 4 + y + d, 8)
        mine = cross.at[rows(s * 4 + y)]
        return remote(mine, mine, s4_send.at[d], s4_recv.at[d], place(x, z, lax.rem(t, 4), lax.div(t, 4)))

    def fourth_from(d):
        t = lax.rem(s * 4 + y - d + 8, 8)
        here = cross.at[rows(t)]
        return remote(here, here, s4_send.at[d], s4_recv.at[d], place(x, z, lax.rem(t, 4), lax.div(t, 4)))

    each(1, 8, lambda d: fourth(d).start())
    each(1, 8, lambda d: fourth_from(d).wait_recv())
    each(1, 32, lambda d: gram_gather_from(d).wait_recv())

    each(1, 32, lambda d: gram_scatter(d).wait_send())
    each(1, 32, lambda d: gram_gather(d).wait_send())
    each(0, CHUNKS, lambda c: across(c).wait_send())
    each(1, NZ, lambda d: third(d).wait_send())
    each(1, 8, lambda d: fourth(d).wait_send())

    @pl.when(s == 0)
    def _():
        for copy in ring_a:
            copy.wait_send()
        for d in range(3):
            second_a(d).wait_send()

    @pl.when(s == 1)
    def _():
        for copy in ring_b:
            copy.wait_send()
        for d in range(3):
            second_b(d).wait_send()


def finish_kernel(voxels, sketch, gram, cross, basis, r_factor, projected, t_ref, diag_ref):
    t_ref[...] = gram[...]
    factor256(t_ref, diag_ref)
    upper, inverse = parts(t_ref, diag_ref)
    scale = jnp.sqrt(F(voxels))
    r_factor[...] = upper / scale
    basis[...] = jnp.dot(sketch[...], jnp.transpose(inverse), precision=HI, preferred_element_type=F) * scale
    full = jnp.dot(inverse, cross[...], precision=HI, preferred_element_type=F)
    first = (lax.rem(lax.axis_index("vox"), NY) * 2 + lax.axis_index("sub")) * 16
    projected[...] = pltpu.roll(full, lax.rem(128 - first, 128), 1)[:, :16]


def local(movie, test_matrix):
    shape = jax.ShapeDtypeStruct
    in_vmem = pl.BlockSpec(memory_space=VMEM)
    sketch, gram, cross = pl.pallas_call(
        reduce_kernel,
        out_shape=(shape((1024, 256), F), shape((32, 8, 256), F), shape((256, 128), F)),
        in_specs=[pl.BlockSpec(memory_space=pl.ANY)] * 2,
        out_specs=[in_vmem] * 3,
        scratch_shapes=[
            VMEM((CHUNKS, 1024, WIDE), jnp.bfloat16),
            VMEM((CHUNKS, WIDE, 256), jnp.bfloat16),
            VMEM((256, 1024), F),
            VMEM((256, 1024), jnp.bfloat16),
            VMEM((CHUNKS, 256, WIDE), F),
            VMEM((CHUNKS, 128, WIDE), F),
            VMEM((CHUNKS, 128, WIDE), F),
            VMEM((32, 8, 256), F),
            VMEM((32, 8, 256), F),
            VMEM((NZ, 8, 256), F),
            VMEM((2, 128, WIDE), F),
            VMEM((2, 2, 128, WIDE), F),
            VMEM((2, 4, 32, WIDE), F),
            VMEM((2, 8, 32, WIDE), F),
            VMEM((2, 128, WIDE), F),
            VMEM((8, 32, WIDE), F),
            VMEM((3, 2, 32, WIDE), F),
            VMEM((2, 32, WIDE), F),
            VMEM((NZ, 32, 128), F),
        ]
        + [DMA((n,)) for n in (8, 8, 8, 8, 32, 32, 8, 8, 32, 32, 6, 6, 3, 3, 8, 8, 8, 8)],
        compiler_params=pltpu.CompilerParams(
            collective_id=0, has_side_effects=True, vmem_limit_bytes=60 * 1024 * 1024
        ),
    )(movie, test_matrix)
    voxels = movie.shape[0] * NX * NY * NZ * 2
    return pl.pallas_call(
        lambda *refs: finish_kernel(voxels, *refs),
        out_shape=(shape((1024, 256), F), shape((256, 256), F), shape((256, 16), F)),
        in_specs=[in_vmem] * 3,
        out_specs=[in_vmem] * 3,
        scratch_shapes=[VMEM((256, 256), F), VMEM((256, 128), F)],
    )(sketch, gram.reshape(256, 256), cross)


def solution(mesh):
    placed = (P(("vox", "sub"), None), P())
    return jax.shard_map(
        local,
        mesh=mesh,
        in_specs=placed,
        out_specs=(P(("vox", "sub"), None), P(), P(None, ("vox", "sub"))),
        check_vma=False,
    )
```

```python
import jax
import jax.numpy as jnp
from jax import lax
from jax.experimental import pallas as pl
from jax.experimental.pallas import tpu as pltpu
from jax.sharding import PartitionSpec as P

F = jnp.float32
HI = lax.Precision.HIGHEST
MESH = pl.DeviceIdType.MESH
VMEM = pltpu.VMEM
DMA = pltpu.SemaphoreType.DMA
NX, NZ, NY = 4, 8, 4
CHUNKS, WIDE = 8, 512


def place(x, z, y, s):
    return ((x * NZ + z) * NY + y, s)


def remote(src, dst, send, recv, device):
    return pltpu.make_async_remote_copy(
        src_ref=src, dst_ref=dst, send_sem=send, recv_sem=recv, device_id=device, device_id_type=MESH
    )


def each(lo, hi, body):
    lax.fori_loop(lo, hi, lambda i, c: (body(i), c)[1], 0)


def factor64(block, left):
    lane = lax.broadcasted_iota(jnp.int32, (8, 8, 128), 2)
    line = lax.broadcasted_iota(jnp.int32, (8, 8, 128), 0) * 8 + lax.broadcasted_iota(jnp.int32, (8, 8, 128), 1)
    sub = lax.broadcasted_iota(jnp.int32, (8, 128), 0)
    here = (lane < 64) if left else (lane >= 64)
    at, eye = (0, 64) if left else (64, 0)
    below = jnp.where(here, block.reshape(8, 8, 128), (lane == eye + line).astype(F))
    done = []
    for p in range(8):
        n = 8 - p
        first = at + 8 * p
        cols = [jnp.broadcast_to(below[:, :, first + j:first + j + 1], (n, 8, 128)) for j in range(8)]
        pivot = jnp.ones((8, 128), F)
        for k in range(8):
            d = jnp.broadcast_to(cols[k][0, k:k + 1, :], (8, 128))
            pivot = jnp.where(sub == k, d, pivot)
            m = cols[k] * (1.0 / d)[None]
            top = jnp.where(sub > k, m[0], 0.0)[None]
            m = jnp.concatenate([top, m[1:]], axis=0) if n > 1 else top
            row = jnp.broadcast_to(below[0, k:k + 1, :], (8, 128))
            for j in range(k + 1, 8):
                u = jnp.broadcast_to(cols[j][0, k:k + 1, :], (8, 128))
                cols[j] = cols[j] - m * u[None]
            below = below - m * row[None]
        done.append(lax.rsqrt(pivot) * below[0])
        below = below[1:]
    out = jnp.stack(done)
    return jnp.where(here & (lane - at < line), 0.0, out).reshape(64, 128)


def factor_block(t_ref, diag_ref, s):
    col = lax.broadcasted_iota(jnp.int32, (64, 256), 1)
    row = lax.broadcasted_iota(jnp.int32, (64, 256), 0)
    r0 = 64 * s
    tile = 128 * (s // 2)
    left = s % 2 == 0
    t = t_ref[r0 : r0 + 64, :]
    both = factor64(t[:, tile : tile + 128], left)
    diag_ref[r0 : r0 + 64, :] = both
    y = jnp.where((col >= r0) & (col < r0 + 64), (col - r0 == row).astype(F), t)
    z = jnp.zeros((64, 256), F)
    us = jnp.dot(both, jnp.concatenate([z, y] if left else [y, z], axis=0), precision=HI, preferred_element_type=F)
    t_ref[r0 : r0 + 64, :] = us
    if s < 3:
        full = lax.dot_general(us, us, (((0,), (0,)), ((), ())), precision=HI, preferred_element_type=F)
        col = lax.broadcasted_iota(jnp.int32, (192 - r0, 256), 1)
        rest = jnp.where((col >= r0) & (col < r0 + 64), 0.0, t_ref[r0 + 64 :, :])
        t_ref[r0 + 64 :, :] = rest - full[r0 + 64 :, :]


def parts(t_ref, diag_ref):
    col = lax.broadcasted_iota(jnp.int32, (256, 256), 1)
    row = lax.broadcasted_iota(jnp.int32, (256, 256), 0)
    t = t_ref[...]
    d = diag_ref[...]
    dd = jnp.concatenate([d, d], axis=1)
    upper = jnp.where(col // 64 == row // 64, dd, t)
    return jnp.where(col >= row, upper, 0.0), jnp.where(col <= row, t, 0.0)


def reduce_kernel(
    movie, test, sketch, upper, inverse, cross,
    mv, tv, skt, skb, part, drecv, half, gpart, grs, gz, gram, t_ref, diag_ref,
    a_tmp, a_in, b_tmp, b_in, pa, pb, r2, p2, r3, p3,
    msem, tsem, dsend, drsem, gs_send, gs_recv, gz_send, gz_recv, ga_send, ga_recv,
    s1_send, s1_recv, s2_send, s2_recv, s3_send, s3_recv, s4_send, s4_recv,
):
    vox, s = lax.axis_index("vox"), lax.axis_index("sub")
    y = lax.rem(vox, NY)
    z = lax.rem(lax.div(vox, NY), NZ)
    x = lax.div(vox, NY * NZ)
    q = (x * NY + y) * 2 + s
    other = place(x, z, y, 1 - s)

    def load(c):
        wide = pl.ds(pl.multiple_of(c * WIDE, WIDE), WIDE)
        return (
            pltpu.make_async_copy(movie.at[:, wide], mv.at[c], msem.at[c]),
            pltpu.make_async_copy(test.at[wide], tv.at[c], tsem.at[c]),
        )

    def start(c):
        for copy in load(c):
            copy.start()

    each(0, CHUNKS, start)

    def plane(d):
        t = lax.rem(q + d, 32)
        return t, place(lax.div(t, NY * 2), z, lax.rem(lax.div(t, 2), NY), lax.rem(t, 2))

    def column(d):
        t = lax.rem(z + d, NZ)
        return t, place(x, t, y, s)

    barrier = pltpu.get_barrier_semaphore()

    def greet(device):
        pl.semaphore_signal(barrier, inc=1, device_id=device, device_id_type=MESH)

    each(1, 32, lambda d: greet(plane(d)[1]))
    each(1, NZ, lambda d: greet(column(d)[1]))

    sketch[...] = jnp.zeros_like(sketch)

    def project(c):
        for copy in load(c):
            copy.wait()
        sketch[...] += jnp.dot(mv[c], tv[c], preferred_element_type=F)

    each(0, CHUNKS, project)
    skt[...] = jnp.transpose(sketch[...])
    skb[...] = skt[...].astype(jnp.bfloat16)
    gpart[...] = jnp.dot(skt[...], sketch[...], precision=HI, preferred_element_type=F).reshape(32, 8, 256)

    pl.semaphore_wait(barrier, 31 + NZ - 1)

    def gram_scatter(d):
        t, device = plane(d)
        return remote(gpart.at[t], grs.at[d], gs_send.at[d], gs_recv.at[d], device)

    each(1, 32, lambda d: gram_scatter(d).start())

    xr, xo, xl = (lax.rem(x + d, NX) for d in (1, 2, 3))
    yr, yo, yl = (lax.rem(y + d, NY) for d in (1, 2, 3))
    right_x, left_x = place(xr, z, y, s), place(xl, z, y, s)
    right_y, left_y = place(x, z, yr, s), place(x, z, yl, s)

    def across(i):
        rows = pl.ds(pl.multiple_of((1 - s) * 128, 128), 128)
        return remote(part.at[i, rows], drecv.at[i], dsend.at[i], drsem.at[i], other)

    def multiply(i):
        part[i] = jnp.dot(skb[...], mv[lax.rem(2 * xo + i, CHUNKS)], preferred_element_type=F)
        across(i).start()

    each(0, CHUNKS, multiply)

    def ring(i, src, dst, device):
        return remote(src, dst, s1_send.at[i], s1_recv.at[i], device)

    lo, hi = pl.ds(0, 4), pl.ds(4, 4)
    ring_a = [
        ring(0, half.at[0, lo], a_tmp.at[0], right_x),
        ring(1, half.at[0, hi], a_tmp.at[1], left_x),
        ring(2, half.at[3, hi], a_in.at[0, hi], right_x),
        ring(3, half.at[1, lo], a_in.at[1, lo], left_x),
        ring(4, half.at[3, lo], a_in.at[0, lo], right_x),
        ring(5, half.at[1, hi], a_in.at[1, hi], left_x),
    ]
    be, af = pl.ds(0, 2), pl.ds(2, 2)
    every = pl.ds(0, NZ)
    ring_b = [
        ring(0, half.at[be, every, yo], b_tmp.at[0], right_y),
        ring(1, half.at[af, every, yo], b_tmp.at[1], left_y),
        ring(2, half.at[af, every, yr], b_in.at[0, af], right_y),
        ring(3, half.at[be, every, yl], b_in.at[1, be], left_y),
        ring(4, half.at[be, every, yr], b_in.at[0, be], right_y),
        ring(5, half.at[af, every, yl], b_in.at[1, af], left_y),
    ]

    def begin(a, b):
        @pl.when(s == 0)
        def _():
            for i in a:
                ring_a[i].start()

        @pl.when(s == 1)
        def _():
            for i in b:
                ring_b[i].start()

    after = {1: ((0, 1), ()), 3: ((3,), (0, 3)), 7: ((2,), (1, 2))}
    for i in range(CHUNKS):
        across(i).wait_recv()
        both = part[i, pl.ds(pl.multiple_of(s * 128, 128), 128)] + drecv[i]
        half[i // 2, pl.ds(4 * (i % 2), 4)] = jnp.transpose(both).reshape(4, NY, 32, 128)
        if i in after:
            begin(*after[i])

    each(1, 32, lambda d: gram_scatter(d).wait_recv())
    total = gpart[q]
    for d in range(1, 32):
        total = total + grs[d]
    gz[z] = total

    def gram_column(d):
        t, device = column(d)
        return remote(gz.at[z], gz.at[z], gz_send.at[d], gz_recv.at[d], device)

    def gram_column_from(d):
        t = lax.rem(z - d + NZ, NZ)
        return remote(gz.at[t], gz.at[t], gz_send.at[d], gz_recv.at[d], place(x, t, y, s))

    each(1, NZ, lambda d: gram_column(d).start())

    @pl.when(s == 0)
    def _():
        ring_a[0].wait_recv()
        half[3, lo] = half[3, lo] + a_tmp[0]
        ring_a[4].start()
        ring_a[1].wait_recv()
        half[1, hi] = half[1, hi] + a_tmp[1]
        ring_a[5].start()

    @pl.when(s == 1)
    def _():
        ring_b[0].wait_recv()
        half[be, every, yr] = half[be, every, yr] + b_tmp[0]
        ring_b[4].start()
        ring_b[1].wait_recv()
        half[af, every, yl] = half[af, every, yl] + b_tmp[1]
        ring_b[5].start()

    each(1, NZ, lambda d: gram_column_from(d).wait_recv())
    each(1, NZ, lambda d: gram_column(d).wait_send())
    total = gz[0]
    for j in range(1, NZ):
        total = total + gz[j]
    gram[q] = total

    def gram_gather(d):
        t, device = plane(d)
        return remote(gram.at[q], gram.at[q], ga_send.at[d], ga_recv.at[d], device)

    def gram_gather_from(d):
        t, device = plane(32 - d)
        return remote(gram.at[t], gram.at[t], ga_send.at[d], ga_recv.at[d], device)

    each(1, 32, lambda d: gram_gather(d).start())

    def second_a(d):
        t = (yr, yo, yl)[d]
        return remote(pa.at[every, t], r2.at[d], s2_send.at[d], s2_recv.at[d], place(x, z, t, s))

    def second_b(d):
        t = (xr, xo, xl)[d]
        return remote(pb.at[(3, 0, 1)[d]], r2.at[d], s2_send.at[d], s2_recv.at[d], place(t, z, y, s))

    @pl.when(s == 0)
    def _():
        for copy in ring_a[2:]:
            copy.wait_recv()
        pa[...] = half[2] + a_in[0] + a_in[1]
        for d in range(3):
            second_a(d).start()

    @pl.when(s == 1)
    def _():
        for copy in ring_b[2:]:
            copy.wait_recv()
        pb[...] = half[:, :, y] + b_in[0] + b_in[1]
        for d in range(3):
            second_b(d).start()

    each(1, 32, lambda d: gram_gather_from(d).wait_recv())
    t_ref[...] = gram[...].reshape(256, 256)
    factor_block(t_ref, diag_ref, 0)

    for d in range(3):
        second_a(d).wait_recv()

    @pl.when(s == 0)
    def _():
        p2[...] = pa[:, y] + r2[0] + r2[1] + r2[2]

    @pl.when(s == 1)
    def _():
        p2[...] = pb[2] + r2[0] + r2[1] + r2[2]

    def third(d):
        t, device = column(d)
        return remote(p2.at[t], r3.at[d], s3_send.at[d], s3_recv.at[d], device)

    each(1, NZ, lambda d: third(d).start())
    for block in range(1, 4):
        factor_block(t_ref, diag_ref, block)
    upper[...], inverse[...] = parts(t_ref, diag_ref)

    each(1, NZ, lambda d: third(d).wait_recv())
    total = p2[z]
    for d in range(1, NZ):
        total = total + r3[d]
    p3[...] = total.reshape(2, 16, 128)
    last = remote(p3.at[1 - s], cross.at[s], s4_send.at[0], s4_recv.at[0], other)
    last.start()
    cross[s] = p3[s]
    remote(p3.at[s], cross.at[1 - s], s4_send.at[0], s4_recv.at[0], other).wait_recv()

    each(1, 32, lambda d: gram_scatter(d).wait_send())
    each(1, 32, lambda d: gram_gather(d).wait_send())
    each(0, CHUNKS, lambda i: across(i).wait_send())
    each(1, NZ, lambda d: third(d).wait_send())
    last.wait_send()

    @pl.when(s == 0)
    def _():
        for copy in ring_a:
            copy.wait_send()
        for d in range(3):
            second_a(d).wait_send()

    @pl.when(s == 1)
    def _():
        for copy in ring_b:
            copy.wait_send()
        for d in range(3):
            second_b(d).wait_send()


def finish_kernel(voxels, sketch, upper, inverse, cross, basis, r_factor, projected):
    scale = jnp.sqrt(F(voxels))
    turned = jnp.transpose(inverse[...])
    r_factor[...] = upper[...] / scale
    basis[...] = jnp.dot(sketch[...], turned, precision=HI, preferred_element_type=F) * scale
    both = jnp.concatenate([cross[0], cross[1]], axis=1)
    projected[...] = jnp.dot(both, turned, precision=HI, preferred_element_type=F)


def local(movie, test_matrix):
    shape = jax.ShapeDtypeStruct
    movie, test_matrix = (pltpu.with_memory_space_constraint(a, pltpu.HBM) for a in (movie, test_matrix))
    in_vmem = pl.BlockSpec(memory_space=VMEM)
    square = shape((256, 256), F)
    sketch, upper, inverse, cross = pl.pallas_call(
        reduce_kernel,
        out_shape=(shape((1024, 256), F), square, square, shape((2, 16, 128), F)),
        in_specs=[pl.BlockSpec(memory_space=pltpu.HBM)] * 2,
        out_specs=[in_vmem] * 4,
        scratch_shapes=[
            VMEM((CHUNKS, 1024, WIDE), jnp.bfloat16),
            VMEM((CHUNKS, WIDE, 256), jnp.bfloat16),
            VMEM((256, 1024), F),
            VMEM((256, 1024), jnp.bfloat16),
            VMEM((CHUNKS, 256, WIDE), F),
            VMEM((CHUNKS, 128, WIDE), F),
            VMEM((NX, NZ, NY, 32, 128), F),
            VMEM((32, 8, 256), F),
            VMEM((32, 8, 256), F),
            VMEM((NZ, 8, 256), F),
            VMEM((32, 8, 256), F),
            VMEM((256, 256), F),
            VMEM((256, 128), F),
            VMEM((2, 4, NY, 32, 128), F),
            VMEM((2, NZ, NY, 32, 128), F),
            VMEM((2, 2, NZ, 32, 128), F),
            VMEM((2, NX, NZ, 32, 128), F),
            VMEM((NZ, NY, 32, 128), F),
            VMEM((NX, NZ, 32, 128), F),
            VMEM((3, NZ, 32, 128), F),
            VMEM((NZ, 32, 128), F),
            VMEM((NZ, 32, 128), F),
            VMEM((2, 16, 128), F),
        ]
        + [DMA((n,)) for n in (8, 8, 8, 8, 32, 32, 8, 8, 32, 32, 6, 6, 3, 3, 8, 8, 1, 1)],
        compiler_params=pltpu.CompilerParams(
            collective_id=0, has_side_effects=True, vmem_limit_bytes=40 * 1024 * 1024
        ),
    )(movie, test_matrix)
    voxels = movie.shape[0] * NX * NY * NZ * 2
    basis, r_factor, projected = pl.pallas_call(
        lambda *refs: finish_kernel(voxels, *refs),
        out_shape=(shape((1024, 256), F), square, shape((16, 256), F)),
        in_specs=[in_vmem] * 4,
        out_specs=[in_vmem] * 3,
        compiler_params=pltpu.CompilerParams(vmem_limit_bytes=16 * 1024 * 1024),
    )(sketch, upper, inverse, cross)
    return basis, r_factor, projected.T


def solution(mesh):
    placed = (P(("vox", "sub"), None), P())
    return jax.shard_map(
        local,
        mesh=mesh,
        in_specs=placed,
        out_specs=(P(("vox", "sub"), None), P(), P(None, ("vox", "sub"))),
        check_vma=False,
    )
```

```python
import jax
import jax.numpy as jnp
from jax import lax
from jax.experimental import pallas as pl
from jax.experimental.pallas import tpu as pltpu
from jax.sharding import PartitionSpec as P

F = jnp.float32
HI = lax.Precision.HIGHEST
MESH = pl.DeviceIdType.MESH
VMEM = pltpu.VMEM
DMA = pltpu.SemaphoreType.DMA
NX, NZ, NY = 4, 8, 4
CHUNKS, WIDE, BLOCK, LAG, PIECES = 8, 512, 256, 4, 24


def place(x, z, y, s):
    return ((x * NZ + z) * NY + y, s)


def remote(src, dst, send, recv, device):
    return pltpu.make_async_remote_copy(
        src_ref=src, dst_ref=dst, send_sem=send, recv_sem=recv, device_id=device, device_id_type=MESH
    )


def each(lo, hi, body):
    lax.fori_loop(lo, hi, lambda i, c: (body(i), c)[1], 0)


def factor64(block, left):
    lane = lax.broadcasted_iota(jnp.int32, (8, 8, 128), 2)
    line = lax.broadcasted_iota(jnp.int32, (8, 8, 128), 0) * 8 + lax.broadcasted_iota(jnp.int32, (8, 8, 128), 1)
    sub = lax.broadcasted_iota(jnp.int32, (8, 128), 0)
    here = (lane < 64) if left else (lane >= 64)
    at, eye = (0, 64) if left else (64, 0)
    below = jnp.where(here, block.reshape(8, 8, 128), (lane == eye + line).astype(F))
    done = []
    for p in range(8):
        n = 8 - p
        first = at + 8 * p
        cols = [jnp.broadcast_to(below[:, :, first + j:first + j + 1], (n, 8, 128)) for j in range(8)]
        pivot = jnp.ones((8, 128), F)
        for k in range(8):
            d = jnp.broadcast_to(cols[k][0, k:k + 1, :], (8, 128))
            pivot = jnp.where(sub == k, d, pivot)
            m = cols[k] * (1.0 / d)[None]
            top = jnp.where(sub > k, m[0], 0.0)[None]
            m = jnp.concatenate([top, m[1:]], axis=0) if n > 1 else top
            row = jnp.broadcast_to(below[0, k:k + 1, :], (8, 128))
            for j in range(k + 1, 8):
                u = jnp.broadcast_to(cols[j][0, k:k + 1, :], (8, 128))
                cols[j] = cols[j] - m * u[None]
            below = below - m * row[None]
        done.append(lax.rsqrt(pivot) * below[0])
        below = below[1:]
    out = jnp.stack(done)
    return jnp.where(here & (lane - at < line), 0.0, out).reshape(64, 128)


def factor_block(t_ref, diag_ref, s):
    col = lax.broadcasted_iota(jnp.int32, (64, 256), 1)
    row = lax.broadcasted_iota(jnp.int32, (64, 256), 0)
    r0 = 64 * s
    tile = 128 * (s // 2)
    left = s % 2 == 0
    t = t_ref[r0 : r0 + 64, :]
    both = factor64(t[:, tile : tile + 128], left)
    diag_ref[r0 : r0 + 64, :] = both
    y = jnp.where((col >= r0) & (col < r0 + 64), (col - r0 == row).astype(F), t)
    z = jnp.zeros((64, 256), F)
    us = jnp.dot(both, jnp.concatenate([z, y] if left else [y, z], axis=0), precision=HI, preferred_element_type=F)
    t_ref[r0 : r0 + 64, :] = us
    if s < 3:
        full = lax.dot_general(us, us, (((0,), (0,)), ((), ())), precision=HI, preferred_element_type=F)
        col = lax.broadcasted_iota(jnp.int32, (192 - r0, 256), 1)
        rest = jnp.where((col >= r0) & (col < r0 + 64), 0.0, t_ref[r0 + 64 :, :])
        t_ref[r0 + 64 :, :] = rest - full[r0 + 64 :, :]


def parts(t_ref, diag_ref):
    col = lax.broadcasted_iota(jnp.int32, (256, 256), 1)
    row = lax.broadcasted_iota(jnp.int32, (256, 256), 0)
    t = t_ref[...]
    d = diag_ref[...]
    dd = jnp.concatenate([d, d], axis=1)
    upper = jnp.where(col // 64 == row // 64, dd, t)
    return jnp.where(col >= row, upper, 0.0), jnp.where(col <= row, t, 0.0)


def reduce_kernel(
    movie, test, pair, upper, inverse, cross,
    mv, tv, turned, grown, part, drecv, half, gpart, grs, gz, gram, t_ref, diag_ref,
    a_tmp, a_in, b_tmp, b_in, pa, pb, r2, p2, r3, p3,
    msem, tsem, dsend, drsem, gs_send, gs_recv, gz_send, gz_recv, ga_send, ga_recv,
    s1_send, s1_recv, s2_send, s2_recv, s3_send, s3_recv, s4_send, s4_recv,
):
    vox, s = lax.axis_index("vox"), lax.axis_index("sub")
    y = lax.rem(vox, NY)
    z = lax.rem(lax.div(vox, NY), NZ)
    x = lax.div(vox, NY * NZ)
    q = (x * NY + y) * 2 + s
    other = place(x, z, y, 1 - s)

    def block(b):
        return pl.ds(pl.multiple_of(b * BLOCK, BLOCK), BLOCK)

    def load(b):
        return pltpu.make_async_copy(movie.at[block(b)], mv.at[block(b)], msem.at[b])

    load_test = pltpu.make_async_copy(test, tv, tsem.at[0])
    load_test.start()
    each(0, 4, lambda b: load(b).start())

    def plane(d):
        t = lax.rem(q + d, 32)
        return t, place(lax.div(t, NY * 2), z, lax.rem(lax.div(t, 2), NY), lax.rem(t, 2))

    def column(d):
        t = lax.rem(z + d, NZ)
        return t, place(x, t, y, s)

    barrier = pltpu.get_barrier_semaphore()

    def greet(device):
        pl.semaphore_signal(barrier, inc=1, device_id=device, device_id_type=MESH)

    each(1, 32, lambda d: greet(plane(d)[1]))
    each(1, NZ, lambda d: greet(column(d)[1]))

    grown[...] = jnp.zeros_like(grown)
    load_test.wait()

    def project(b):
        load(b).wait()
        sketch = jnp.dot(mv[block(b)], tv[...], preferred_element_type=F)
        near = sketch.astype(jnp.bfloat16)
        both = jnp.concatenate([near, (sketch - near.astype(F)).astype(jnp.bfloat16)], axis=1)
        pair[block(b)] = both
        across = jnp.transpose(both)
        turned[:, block(b)] = across
        grown[...] += jnp.dot(across, both, preferred_element_type=F)

    each(0, 4, project)
    low, high = slice(0, 256), slice(256, 512)
    product = (grown[low, low] + grown[high, high]) + (grown[low, high] + grown[high, low])
    top, bottom = slice(0, 128), slice(128, 256)
    quarters = ((top, top), (top, bottom), (bottom, bottom))
    for i, (a, b) in enumerate(quarters):
        gpart[8 * i : 8 * i + 8] = product[a, b].reshape(8, 16, 128)

    xr, xo, xl = (lax.rem(x + d, NX) for d in (1, 2, 3))
    yr, yo, yl = (lax.rem(y + d, NY) for d in (1, 2, 3))
    right_x, left_x = place(xr, z, y, s), place(xl, z, y, s)
    right_y, left_y = place(x, z, yr, s), place(x, z, yl, s)

    turn = lax.rem(x + y, 4)
    owner = turn < 3
    mine = (x * 3 + lax.min(turn, 2)) * 2 + s

    def others(body):
        def visit(j):
            t = lax.rem(mine + j, PIECES)
            tx, ts = lax.div(t, 6), lax.rem(t, 2)
            ty = lax.rem(lax.rem(lax.div(t, 2), 3) - tx + 4, 4)
            at = (tx * NY + ty) * 2 + ts

            @pl.when(at != q)
            def _():
                body(t, at, place(tx, z, ty, ts))

        each(0, PIECES, visit)

    pl.semaphore_wait(barrier, 31 + NZ - 1)

    def gram_scatter(t, at, device):
        d = lax.rem(at - q + 32, 32)
        return remote(gpart.at[t], grs.at[d], gs_send.at[t], gs_recv.at[d], device)

    others(lambda *a: gram_scatter(*a).start())

    def across(i):
        rows = pl.ds(pl.multiple_of((1 - s) * 128, 128), 128)
        return remote(part.at[i, rows], drecv.at[i], dsend.at[i], drsem.at[i], other)

    def multiply(i):
        h, r = i // 4, i % 4
        first = pl.multiple_of((2 * lax.rem(xo + r, NX) + h) * WIDE, WIDE)
        part[i] = jnp.dot(turned[low], mv[:, pl.ds(first, WIDE)], preferred_element_type=F)
        across(i).start()

    be, af, every = pl.ds(0, 2), pl.ds(2, 2), pl.ds(0, 4)

    def ring(h, i, src, dst, device):
        return remote(src, dst, s1_send.at[h, i], s1_recv.at[h, i], device)

    ring_a = [
        [
            ring(h, 0, half.at[h, 0, be], a_tmp.at[h, 0], right_x),
            ring(h, 1, half.at[h, 0, af], a_tmp.at[h, 1], left_x),
            ring(h, 2, half.at[h, 3, af], a_in.at[h, 0, af], right_x),
            ring(h, 3, half.at[h, 1, be], a_in.at[h, 1, be], left_x),
            ring(h, 4, half.at[h, 3, be], a_in.at[h, 0, be], right_x),
            ring(h, 5, half.at[h, 1, af], a_in.at[h, 1, af], left_x),
        ]
        for h in range(2)
    ]
    ring_b = [
        [
            ring(h, 0, half.at[h, be, every, yo], b_tmp.at[h, 0], right_y),
            ring(h, 1, half.at[h, af, every, yo], b_tmp.at[h, 1], left_y),
            ring(h, 2, half.at[h, af, every, yr], b_in.at[h, 0, af], right_y),
            ring(h, 3, half.at[h, be, every, yl], b_in.at[h, 1, be], left_y),
            ring(h, 4, half.at[h, be, every, yr], b_in.at[h, 0, be], right_y),
            ring(h, 5, half.at[h, af, every, yl], b_in.at[h, 1, af], left_y),
        ]
        for h in range(2)
    ]

    def begin(h, a, b):
        @pl.when(s == 0)
        def _():
            for i in a:
                ring_a[h][i].start()

        @pl.when(s == 1)
        def _():
            for i in b:
                ring_b[h][i].start()

    after = {0: ((0, 1), ()), 1: ((3,), (0, 3)), 3: ((2,), (1, 2))}
    for step in range(CHUNKS + LAG):
        if step < CHUNKS:
            multiply(step)
        i = step - LAG
        if i >= 0:
            across(i).wait_recv()
            both = part[i, pl.ds(pl.multiple_of(s * 128, 128), 128)] + drecv[i]
            half[i // 4, i % 4] = jnp.transpose(both).reshape(4, NY, 32, 128)
            if i % 4 in after:
                begin(i // 4, *after[i % 4])

    def ring_again(h):
        @pl.when(s == 0)
        def _():
            ring_a[h][0].wait_recv()
            half[h, 3, be] = half[h, 3, be] + a_tmp[h, 0]
            ring_a[h][4].start()
            ring_a[h][1].wait_recv()
            half[h, 1, af] = half[h, 1, af] + a_tmp[h, 1]
            ring_a[h][5].start()

        @pl.when(s == 1)
        def _():
            ring_b[h][0].wait_recv()
            half[h, be, every, yr] = half[h, be, every, yr] + b_tmp[h, 0]
            ring_b[h][4].start()
            ring_b[h][1].wait_recv()
            half[h, af, every, yl] = half[h, af, every, yl] + b_tmp[h, 1]
            ring_b[h][5].start()

    def second_a(h, d):
        t = (yr, yo, yl)[d]
        return remote(pa.at[h, every, t], r2.at[h, d], s2_send.at[h, d], s2_recv.at[h, d], place(x, z, t, s))

    def second_b(h, d):
        t = (xr, xo, xl)[d]
        return remote(pb.at[h, (3, 0, 1)[d]], r2.at[h, d], s2_send.at[h, d], s2_recv.at[h, d], place(t, z, y, s))

    def second(h):
        @pl.when(s == 0)
        def _():
            for copy in ring_a[h][2:]:
                copy.wait_recv()
            pa[h] = half[h, 2] + a_in[h, 0] + a_in[h, 1]
            for d in range(3):
                second_a(h, d).start()

        @pl.when(s == 1)
        def _():
            for copy in ring_b[h][2:]:
                copy.wait_recv()
            pb[h] = half[h, :, :, y] + b_in[h, 0] + b_in[h, 1]
            for d in range(3):
                second_b(h, d).start()

    def third(d):
        t, device = column(d)
        return remote(p2.at[t], r3.at[d], s3_send.at[d], s3_recv.at[d], device)

    def third_start(h):
        for d in range(3):
            second_a(h, d).wait_recv()

        @pl.when(s == 0)
        def _():
            p2[4 * h : 4 * h + 4] = pa[h, :, y] + r2[h, 0] + r2[h, 1] + r2[h, 2]

        @pl.when(s == 1)
        def _():
            p2[4 * h : 4 * h + 4] = pb[h, 2] + r2[h, 0] + r2[h, 1] + r2[h, 2]

        def visit(d):
            @pl.when(lax.div(column(d)[0], 4) == h)
            def _():
                third(d).start()

        each(1, NZ, visit)

    def gram_column(d):
        t, device = column(d)
        return remote(gz.at[z], gz.at[z], gz_send.at[d], gz_recv.at[d], device)

    def gram_column_from(d):
        t = lax.rem(z - d + NZ, NZ)
        return remote(gz.at[t], gz.at[t], gz_send.at[d], gz_recv.at[d], place(x, t, y, s))

    def gram_gather(d):
        return remote(gram.at[mine], gram.at[mine], ga_send.at[d], ga_recv.at[mine], plane(d)[1])

    def gram_gather_from(t, at, device):
        return remote(gram.at[t], gram.at[t], ga_send.at[0], ga_recv.at[t], device)

    ring_again(0)

    @pl.when(owner)
    def _():
        each(1, 32, lambda d: remote(gpart.at[0], grs.at[d], gs_send.at[0], gs_recv.at[d], other).wait_recv())
        total = gpart[mine]
        for d in range(1, 32):
            total = total + grs[d]
        gz[z] = total
        each(1, NZ, lambda d: gram_column(d).start())

    ring_again(1)
    second(0)

    @pl.when(owner)
    def _():
        each(1, NZ, lambda d: gram_column_from(d).wait_recv())
        each(1, NZ, lambda d: gram_column(d).wait_send())
        total = gz[0]
        for j in range(1, NZ):
            total = total + gz[j]
        gram[mine] = total
        each(1, 32, lambda d: gram_gather(d).start())

    second(1)
    third_start(0)
    third_start(1)

    others(lambda *a: gram_gather_from(*a).wait_recv())
    t_ref[bottom, top] = jnp.zeros((128, 128), F)
    for i, (a, b) in enumerate(quarters):
        t_ref[a, b] = gram[8 * i : 8 * i + 8].reshape(128, 128)
    for block in range(4):
        factor_block(t_ref, diag_ref, block)
    upper[...], inverse[...] = parts(t_ref, diag_ref)

    each(1, NZ, lambda d: third(d).wait_recv())
    total = p2[z]
    for d in range(1, NZ):
        total = total + r3[d]
    p3[...] = total.reshape(2, 16, 128)
    last = remote(p3.at[1 - s], cross.at[s], s4_send.at[0], s4_recv.at[0], other)
    last.start()
    cross[s] = p3[s]
    remote(p3.at[s], cross.at[1 - s], s4_send.at[0], s4_recv.at[0], other).wait_recv()

    others(lambda *a: gram_scatter(*a).wait_send())

    @pl.when(owner)
    def _():
        each(1, 32, lambda d: gram_gather(d).wait_send())

    each(0, CHUNKS, lambda i: across(i).wait_send())
    each(1, NZ, lambda d: third(d).wait_send())
    last.wait_send()

    @pl.when(s == 0)
    def _():
        for h in range(2):
            for copy in ring_a[h]:
                copy.wait_send()
            for d in range(3):
                second_a(h, d).wait_send()

    @pl.when(s == 1)
    def _():
        for h in range(2):
            for copy in ring_b[h]:
                copy.wait_send()
            for d in range(3):
                second_b(h, d).wait_send()


def finish_kernel(voxels, pair, upper, inverse, cross, basis, r_factor, projected):
    scale = jnp.sqrt(F(voxels))
    turned = jnp.transpose(inverse[...])
    scaled = turned * scale
    near = scaled.astype(jnp.bfloat16)
    rest = (scaled - near.astype(F)).astype(jnp.bfloat16)
    basis[...] = jnp.dot(pair[...], jnp.concatenate([near, near], axis=0), preferred_element_type=F) + jnp.dot(
        pair[:, :256], rest, preferred_element_type=F
    )
    r_factor[...] = upper[...] / scale
    both = jnp.concatenate([cross[0], cross[1]], axis=1)
    projected[...] = jnp.dot(both, turned, precision=HI, preferred_element_type=F)


def local(movie, test_matrix):
    shape = jax.ShapeDtypeStruct
    movie, test_matrix = (pltpu.with_memory_space_constraint(a, pltpu.HBM) for a in (movie, test_matrix))
    in_vmem = pl.BlockSpec(memory_space=VMEM)
    square = shape((256, 256), F)
    pair, upper, inverse, cross = pl.pallas_call(
        reduce_kernel,
        out_shape=(shape((1024, 512), jnp.bfloat16), square, square, shape((2, 16, 128), F)),
        in_specs=[pl.BlockSpec(memory_space=pltpu.HBM)] * 2,
        out_specs=[in_vmem] * 4,
        scratch_shapes=[
            VMEM((1024, 4096), jnp.bfloat16),
            VMEM((4096, 256), jnp.bfloat16),
            VMEM((512, 1024), jnp.bfloat16),
            VMEM((512, 512), F),
            VMEM((CHUNKS, 256, WIDE), F),
            VMEM((CHUNKS, 128, WIDE), F),
            VMEM((2, NX, 4, NY, 32, 128), F),
            VMEM((PIECES, 16, 128), F),
            VMEM((32, 16, 128), F),
            VMEM((NZ, 16, 128), F),
            VMEM((PIECES, 16, 128), F),
            VMEM((256, 256), F),
            VMEM((256, 128), F),
            VMEM((2, 2, 2, NY, 32, 128), F),
            VMEM((2, 2, 4, NY, 32, 128), F),
            VMEM((2, 2, 2, 4, 32, 128), F),
            VMEM((2, 2, NX, 4, 32, 128), F),
            VMEM((2, 4, NY, 32, 128), F),
            VMEM((2, NX, 4, 32, 128), F),
            VMEM((2, 3, 4, 32, 128), F),
            VMEM((NZ, 32, 128), F),
            VMEM((NZ, 32, 128), F),
            VMEM((2, 16, 128), F),
        ]
        + [DMA((n,)) for n in (4, 1, 8, 8, PIECES, 32, 8, 8, 32, PIECES)]
        + [DMA(n) for n in ((2, 6), (2, 6), (2, 3), (2, 3), (8,), (8,), (1,), (1,))],
        compiler_params=pltpu.CompilerParams(
            collective_id=0, has_side_effects=True, vmem_limit_bytes=40 * 1024 * 1024
        ),
    )(movie, test_matrix)
    voxels = movie.shape[0] * NX * NY * NZ * 2
    basis, r_factor, projected = pl.pallas_call(
        lambda *refs: finish_kernel(voxels, *refs),
        out_shape=(shape((1024, 256), F), square, shape((16, 256), F)),
        in_specs=[in_vmem] * 4,
        out_specs=[in_vmem] * 3,
        compiler_params=pltpu.CompilerParams(vmem_limit_bytes=16 * 1024 * 1024),
    )(pair, upper, inverse, cross)
    return basis, r_factor, projected.T


def solution(mesh):
    placed = (P(("vox", "sub"), None), P())
    return jax.shard_map(
        local,
        mesh=mesh,
        in_specs=placed,
        out_specs=(P(("vox", "sub"), None), P(), P(None, ("vox", "sub"))),
        check_vma=False,
    )
```

```python
import jax
import jax.numpy as jnp
from jax import lax
from jax.experimental import pallas as pl
from jax.experimental.pallas import tpu as pltpu
from jax.sharding import PartitionSpec as P

F = jnp.float32
HI = lax.Precision.HIGHEST
MESH = pl.DeviceIdType.MESH
VMEM = pltpu.VMEM
DMA = pltpu.SemaphoreType.DMA
NX, NZ, NY = 4, 8, 4
CHUNKS, WIDE, LAG, PIECES = 8, 512, 4, 24


def place(x, z, y, s):
    return ((x * NZ + z) * NY + y, s)


def remote(src, dst, send, recv, device):
    return pltpu.make_async_remote_copy(
        src_ref=src, dst_ref=dst, send_sem=send, recv_sem=recv, device_id=device, device_id_type=MESH
    )


def each(lo, hi, body):
    lax.fori_loop(lo, hi, lambda i, c: (body(i), c)[1], 0)


def factor64(block, left):
    lane = lax.broadcasted_iota(jnp.int32, (8, 8, 128), 2)
    line = lax.broadcasted_iota(jnp.int32, (8, 8, 128), 0) * 8 + lax.broadcasted_iota(jnp.int32, (8, 8, 128), 1)
    sub = lax.broadcasted_iota(jnp.int32, (8, 128), 0)
    here = (lane < 64) if left else (lane >= 64)
    at, eye = (0, 64) if left else (64, 0)
    below = jnp.where(here, block.reshape(8, 8, 128), (lane == eye + line).astype(F))
    done = []
    for p in range(8):
        n = 8 - p
        first = at + 8 * p
        cols = [jnp.broadcast_to(below[:, :, first + j:first + j + 1], (n, 8, 128)) for j in range(8)]
        pivot = jnp.ones((8, 128), F)
        for k in range(8):
            d = jnp.broadcast_to(cols[k][0, k:k + 1, :], (8, 128))
            pivot = jnp.where(sub == k, d, pivot)
            m = cols[k] * (1.0 / d)[None]
            top = jnp.where(sub > k, m[0], 0.0)[None]
            m = jnp.concatenate([top, m[1:]], axis=0) if n > 1 else top
            row = jnp.broadcast_to(below[0, k:k + 1, :], (8, 128))
            for j in range(k + 1, 8):
                u = jnp.broadcast_to(cols[j][0, k:k + 1, :], (8, 128))
                cols[j] = cols[j] - m * u[None]
            below = below - m * row[None]
        done.append(lax.rsqrt(pivot) * below[0])
        below = below[1:]
    out = jnp.stack(done)
    return jnp.where(here & (lane - at < line), 0.0, out).reshape(64, 128)


def factor_block(t_ref, diag_ref, s):
    col = lax.broadcasted_iota(jnp.int32, (64, 256), 1)
    row = lax.broadcasted_iota(jnp.int32, (64, 256), 0)
    r0 = 64 * s
    tile = 128 * (s // 2)
    left = s % 2 == 0
    t = t_ref[r0 : r0 + 64, :]
    both = factor64(t[:, tile : tile + 128], left)
    diag_ref[r0 : r0 + 64, :] = both
    y = jnp.where((col >= r0) & (col < r0 + 64), (col - r0 == row).astype(F), t)
    z = jnp.zeros((64, 256), F)
    us = jnp.dot(both, jnp.concatenate([z, y] if left else [y, z], axis=0), precision=HI, preferred_element_type=F)
    t_ref[r0 : r0 + 64, :] = us
    if s < 3:
        full = lax.dot_general(us, us, (((0,), (0,)), ((), ())), precision=HI, preferred_element_type=F)
        col = lax.broadcasted_iota(jnp.int32, (192 - r0, 256), 1)
        rest = jnp.where((col >= r0) & (col < r0 + 64), 0.0, t_ref[r0 + 64 :, :])
        t_ref[r0 + 64 :, :] = rest - full[r0 + 64 :, :]


def parts(t_ref, diag_ref):
    col = lax.broadcasted_iota(jnp.int32, (256, 256), 1)
    row = lax.broadcasted_iota(jnp.int32, (256, 256), 0)
    t = t_ref[...]
    d = diag_ref[...]
    dd = jnp.concatenate([d, d], axis=1)
    upper = jnp.where(col // 64 == row // 64, dd, t)
    return jnp.where(col >= row, upper, 0.0), jnp.where(col <= row, t, 0.0)


def reduce_kernel(
    movie, test, pair, upper, inverse, cross,
    mv, tv, sketch, turned, grown, part, drecv, half, gpart, grs, gz, gram, t_ref, diag_ref,
    a_tmp, a_in, b_tmp, b_in, pa, pb, r2, p2, r3, p3,
    msem, tsem, dsend, drsem, gs_send, gs_recv, gz_send, gz_recv, ga_send, ga_recv,
    s1_send, s1_recv, s2_send, s2_recv, s3_send, s3_recv, s4_send, s4_recv,
):
    vox, s = lax.axis_index("vox"), lax.axis_index("sub")
    y = lax.rem(vox, NY)
    z = lax.rem(lax.div(vox, NY), NZ)
    x = lax.div(vox, NY * NZ)
    q = (x * NY + y) * 2 + s
    other = place(x, z, y, 1 - s)

    def load(c):
        wide = pl.ds(pl.multiple_of(c * WIDE, WIDE), WIDE)
        return (
            pltpu.make_async_copy(movie.at[:, wide], mv.at[c], msem.at[c]),
            pltpu.make_async_copy(test.at[wide], tv.at[c], tsem.at[c]),
        )

    def start(c):
        for copy in load(c):
            copy.start()

    each(0, CHUNKS, start)

    def plane(d):
        t = lax.rem(q + d, 32)
        return t, place(lax.div(t, NY * 2), z, lax.rem(lax.div(t, 2), NY), lax.rem(t, 2))

    def column(d):
        t = lax.rem(z + d, NZ)
        return t, place(x, t, y, s)

    barrier = pltpu.get_barrier_semaphore()

    def greet(device):
        pl.semaphore_signal(barrier, inc=1, device_id=device, device_id_type=MESH)

    each(1, 32, lambda d: greet(plane(d)[1]))
    each(1, NZ, lambda d: greet(column(d)[1]))

    sketch[...] = jnp.zeros_like(sketch)

    def project(c):
        for copy in load(c):
            copy.wait()
        sketch[...] += jnp.dot(mv[c], tv[c], preferred_element_type=F)

    each(0, CHUNKS, project)
    near = sketch[...].astype(jnp.bfloat16)
    pair[...] = jnp.concatenate([near, (sketch[...] - near.astype(F)).astype(jnp.bfloat16)], axis=1)
    turned[...] = jnp.transpose(pair[...])
    grown[...] = jnp.dot(turned[...], pair[...], preferred_element_type=F)
    low, high = slice(0, 256), slice(256, 512)
    product = (grown[low, low] + grown[high, high]) + (grown[low, high] + grown[high, low])
    top, bottom = slice(0, 128), slice(128, 256)
    quarters = ((top, top), (top, bottom), (bottom, bottom))
    for i, (a, b) in enumerate(quarters):
        gpart[8 * i : 8 * i + 8] = product[a, b].reshape(8, 16, 128)

    xr, xo, xl = (lax.rem(x + d, NX) for d in (1, 2, 3))
    yr, yo, yl = (lax.rem(y + d, NY) for d in (1, 2, 3))
    right_x, left_x = place(xr, z, y, s), place(xl, z, y, s)
    right_y, left_y = place(x, z, yr, s), place(x, z, yl, s)

    turn = lax.rem(x + y, 4)
    owner = turn < 3
    mine = (x * 3 + lax.min(turn, 2)) * 2 + s

    def others(body):
        def visit(j):
            t = lax.rem(mine + j, PIECES)
            tx, ts = lax.div(t, 6), lax.rem(t, 2)
            ty = lax.rem(lax.rem(lax.div(t, 2), 3) - tx + 4, 4)
            at = (tx * NY + ty) * 2 + ts

            @pl.when(at != q)
            def _():
                body(t, at, place(tx, z, ty, ts))

        each(0, PIECES, visit)

    pl.semaphore_wait(barrier, 31 + NZ - 1)

    def gram_scatter(t, at, device):
        d = lax.rem(at - q + 32, 32)
        return remote(gpart.at[t], grs.at[d], gs_send.at[t], gs_recv.at[d], device)

    others(lambda *a: gram_scatter(*a).start())

    def across(i):
        rows = pl.ds(pl.multiple_of((1 - s) * 128, 128), 128)
        return remote(part.at[i, rows], drecv.at[i], dsend.at[i], drsem.at[i], other)

    def multiply(i):
        h, r = i // 4, i % 4
        chunk = 2 * lax.rem(xo + r, NX) + h
        part[i] = jnp.dot(turned[low], mv[chunk], preferred_element_type=F)
        across(i).start()

    be, af, every = pl.ds(0, 2), pl.ds(2, 2), pl.ds(0, 4)

    def ring(h, i, src, dst, device):
        return remote(src, dst, s1_send.at[h, i], s1_recv.at[h, i], device)

    ring_a = [
        [
            ring(h, 0, half.at[h, 0, be], a_tmp.at[h, 0], right_x),
            ring(h, 1, half.at[h, 0, af], a_tmp.at[h, 1], left_x),
            ring(h, 2, half.at[h, 3, af], a_in.at[h, 0, af], right_x),
            ring(h, 3, half.at[h, 1, be], a_in.at[h, 1, be], left_x),
            ring(h, 4, half.at[h, 3, be], a_in.at[h, 0, be], right_x),
            ring(h, 5, half.at[h, 1, af], a_in.at[h, 1, af], left_x),
        ]
        for h in range(2)
    ]
    ring_b = [
        [
            ring(h, 0, half.at[h, be, every, yo], b_tmp.at[h, 0], right_y),
            ring(h, 1, half.at[h, af, every, yo], b_tmp.at[h, 1], left_y),
            ring(h, 2, half.at[h, af, every, yr], b_in.at[h, 0, af], right_y),
            ring(h, 3, half.at[h, be, every, yl], b_in.at[h, 1, be], left_y),
            ring(h, 4, half.at[h, be, every, yr], b_in.at[h, 0, be], right_y),
            ring(h, 5, half.at[h, af, every, yl], b_in.at[h, 1, af], left_y),
        ]
        for h in range(2)
    ]

    def begin(h, a, b):
        @pl.when(s == 0)
        def _():
            for i in a:
                ring_a[h][i].start()

        @pl.when(s == 1)
        def _():
            for i in b:
                ring_b[h][i].start()

    after = {0: ((0, 1), ()), 1: ((3,), (0, 3)), 3: ((2,), (1, 2))}
    for step in range(CHUNKS + LAG):
        if step < CHUNKS:
            multiply(step)
        i = step - LAG
        if i >= 0:
            across(i).wait_recv()
            both = part[i, pl.ds(pl.multiple_of(s * 128, 128), 128)] + drecv[i]
            half[i // 4, i % 4] = jnp.transpose(both).reshape(4, NY, 32, 128)
            if i % 4 in after:
                begin(i // 4, *after[i % 4])

    def ring_again(h):
        @pl.when(s == 0)
        def _():
            ring_a[h][0].wait_recv()
            half[h, 3, be] = half[h, 3, be] + a_tmp[h, 0]
            ring_a[h][4].start()
            ring_a[h][1].wait_recv()
            half[h, 1, af] = half[h, 1, af] + a_tmp[h, 1]
            ring_a[h][5].start()

        @pl.when(s == 1)
        def _():
            ring_b[h][0].wait_recv()
            half[h, be, every, yr] = half[h, be, every, yr] + b_tmp[h, 0]
            ring_b[h][4].start()
            ring_b[h][1].wait_recv()
            half[h, af, every, yl] = half[h, af, every, yl] + b_tmp[h, 1]
            ring_b[h][5].start()

    def second_a(h, d):
        t = (yr, yo, yl)[d]
        return remote(pa.at[h, every, t], r2.at[h, d], s2_send.at[h, d], s2_recv.at[h, d], place(x, z, t, s))

    def second_b(h, d):
        t = (xr, xo, xl)[d]
        return remote(pb.at[h, (3, 0, 1)[d]], r2.at[h, d], s2_send.at[h, d], s2_recv.at[h, d], place(t, z, y, s))

    def second(h):
        @pl.when(s == 0)
        def _():
            for copy in ring_a[h][2:]:
                copy.wait_recv()
            pa[h] = half[h, 2] + a_in[h, 0] + a_in[h, 1]
            for d in range(3):
                second_a(h, d).start()

        @pl.when(s == 1)
        def _():
            for copy in ring_b[h][2:]:
                copy.wait_recv()
            pb[h] = half[h, :, :, y] + b_in[h, 0] + b_in[h, 1]
            for d in range(3):
                second_b(h, d).start()

    def third(d):
        t, device = column(d)
        return remote(p2.at[t], r3.at[d], s3_send.at[d], s3_recv.at[d], device)

    def third_start(h):
        for d in range(3):
            second_a(h, d).wait_recv()

        @pl.when(s == 0)
        def _():
            p2[4 * h : 4 * h + 4] = pa[h, :, y] + r2[h, 0] + r2[h, 1] + r2[h, 2]

        @pl.when(s == 1)
        def _():
            p2[4 * h : 4 * h + 4] = pb[h, 2] + r2[h, 0] + r2[h, 1] + r2[h, 2]

        def visit(d):
            @pl.when(lax.div(column(d)[0], 4) == h)
            def _():
                third(d).start()

        each(1, NZ, visit)

    def gram_column(d):
        t, device = column(d)
        return remote(gz.at[z], gz.at[z], gz_send.at[d], gz_recv.at[d], device)

    def gram_column_from(d):
        t = lax.rem(z - d + NZ, NZ)
        return remote(gz.at[t], gz.at[t], gz_send.at[d], gz_recv.at[d], place(x, t, y, s))

    def gram_gather(d):
        return remote(gram.at[mine], gram.at[mine], ga_send.at[d], ga_recv.at[mine], plane(d)[1])

    def gram_gather_from(t, at, device):
        return remote(gram.at[t], gram.at[t], ga_send.at[0], ga_recv.at[t], device)

    def gram_pieces():
        @pl.when(owner)
        def _():
            each(1, 32, lambda d: remote(gpart.at[0], grs.at[d], gs_send.at[0], gs_recv.at[d], other).wait_recv())
            total = gpart[mine]
            for d in range(1, 32):
                total = total + grs[d]
            gz[z] = total
            each(1, NZ, lambda d: gram_column(d).start())

    def gram_totals():
        @pl.when(owner)
        def _():
            each(1, NZ, lambda d: gram_column_from(d).wait_recv())
            each(1, NZ, lambda d: gram_column(d).wait_send())
            total = gz[0]
            for j in range(1, NZ):
                total = total + gz[j]
            gram[mine] = total
            each(1, 32, lambda d: gram_gather(d).start())

    def gram_whole():
        others(lambda *a: gram_gather_from(*a).wait_recv())
        t_ref[bottom, top] = jnp.zeros((128, 128), F)
        for i, (a, b) in enumerate(quarters):
            t_ref[a, b] = gram[8 * i : 8 * i + 8].reshape(128, 128)

    def factor(block):
        factor_block(t_ref, diag_ref, block)

    gram_pieces()
    ring_again(0)
    ring_again(1)
    gram_totals()
    second(0)
    second(1)
    third_start(0)
    gram_whole()
    factor(0)
    third_start(1)
    for block in range(1, 4):
        factor(block)
    upper[...], inverse[...] = parts(t_ref, diag_ref)

    each(1, NZ, lambda d: third(d).wait_recv())
    total = p2[z]
    for d in range(1, NZ):
        total = total + r3[d]
    p3[...] = total.reshape(2, 16, 128)
    last = remote(p3.at[1 - s], cross.at[s], s4_send.at[0], s4_recv.at[0], other)
    last.start()
    cross[s] = p3[s]
    remote(p3.at[s], cross.at[1 - s], s4_send.at[0], s4_recv.at[0], other).wait_recv()

    others(lambda *a: gram_scatter(*a).wait_send())

    @pl.when(owner)
    def _():
        each(1, 32, lambda d: gram_gather(d).wait_send())

    each(0, CHUNKS, lambda i: across(i).wait_send())
    each(1, NZ, lambda d: third(d).wait_send())
    last.wait_send()

    @pl.when(s == 0)
    def _():
        for h in range(2):
            for copy in ring_a[h]:
                copy.wait_send()
            for d in range(3):
                second_a(h, d).wait_send()

    @pl.when(s == 1)
    def _():
        for h in range(2):
            for copy in ring_b[h]:
                copy.wait_send()
            for d in range(3):
                second_b(h, d).wait_send()


def finish_kernel(voxels, pair, upper, inverse, cross, basis, r_factor, projected):
    scale = jnp.sqrt(F(voxels))
    turned = jnp.transpose(inverse[...])
    scaled = turned * scale
    near = scaled.astype(jnp.bfloat16)
    rest = (scaled - near.astype(F)).astype(jnp.bfloat16)
    basis[...] = jnp.dot(pair[...], jnp.concatenate([near, near], axis=0), preferred_element_type=F) + jnp.dot(
        pair[:, :256], rest, preferred_element_type=F
    )
    r_factor[...] = upper[...] / scale
    both = jnp.concatenate([cross[0], cross[1]], axis=1)
    projected[...] = jnp.dot(both, turned, precision=HI, preferred_element_type=F)


def local(movie, test_matrix):
    shape = jax.ShapeDtypeStruct
    movie, test_matrix = (pltpu.with_memory_space_constraint(a, pltpu.HBM) for a in (movie, test_matrix))
    in_vmem = pl.BlockSpec(memory_space=VMEM)
    square = shape((256, 256), F)
    pair, upper, inverse, cross = pl.pallas_call(
        reduce_kernel,
        out_shape=(shape((1024, 512), jnp.bfloat16), square, square, shape((2, 16, 128), F)),
        in_specs=[pl.BlockSpec(memory_space=pltpu.HBM)] * 2,
        out_specs=[in_vmem] * 4,
        scratch_shapes=[
            VMEM((CHUNKS, 1024, WIDE), jnp.bfloat16),
            VMEM((CHUNKS, WIDE, 256), jnp.bfloat16),
            VMEM((1024, 256), F),
            VMEM((512, 1024), jnp.bfloat16),
            VMEM((512, 512), F),
            VMEM((CHUNKS, 256, WIDE), F),
            VMEM((CHUNKS, 128, WIDE), F),
            VMEM((2, NX, 4, NY, 32, 128), F),
            VMEM((PIECES, 16, 128), F),
            VMEM((32, 16, 128), F),
            VMEM((NZ, 16, 128), F),
            VMEM((PIECES, 16, 128), F),
            VMEM((256, 256), F),
            VMEM((256, 128), F),
            VMEM((2, 2, 2, NY, 32, 128), F),
            VMEM((2, 2, 4, NY, 32, 128), F),
            VMEM((2, 2, 2, 4, 32, 128), F),
            VMEM((2, 2, NX, 4, 32, 128), F),
            VMEM((2, 4, NY, 32, 128), F),
            VMEM((2, NX, 4, 32, 128), F),
            VMEM((2, 3, 4, 32, 128), F),
            VMEM((NZ, 32, 128), F),
            VMEM((NZ, 32, 128), F),
            VMEM((2, 16, 128), F),
        ]
        + [DMA((n,)) for n in (8, 8, 8, 8, PIECES, 32, 8, 8, 32, PIECES)]
        + [DMA(n) for n in ((2, 6), (2, 6), (2, 3), (2, 3), (8,), (8,), (1,), (1,))],
        compiler_params=pltpu.CompilerParams(
            collective_id=0, has_side_effects=True, vmem_limit_bytes=40 * 1024 * 1024
        ),
    )(movie, test_matrix)
    voxels = movie.shape[0] * NX * NY * NZ * 2
    basis, r_factor, projected = pl.pallas_call(
        lambda *refs: finish_kernel(voxels, *refs),
        out_shape=(shape((1024, 256), F), square, shape((16, 256), F)),
        in_specs=[in_vmem] * 4,
        out_specs=[in_vmem] * 3,
        compiler_params=pltpu.CompilerParams(vmem_limit_bytes=16 * 1024 * 1024),
    )(pair, upper, inverse, cross)
    return basis, r_factor, projected.T


def solution(mesh):
    placed = (P(("vox", "sub"), None), P())
    return jax.shard_map(
        local,
        mesh=mesh,
        in_specs=placed,
        out_specs=(P(("vox", "sub"), None), P(), P(None, ("vox", "sub"))),
        check_vma=False,
    )
```

```python
import jax
import jax.numpy as jnp
from jax import lax
from jax.experimental import pallas as pl
from jax.experimental.pallas import tpu as pltpu
from jax.sharding import PartitionSpec as P

F = jnp.float32
HI = lax.Precision.HIGHEST
MESH = pl.DeviceIdType.MESH
VMEM = pltpu.VMEM
DMA = pltpu.SemaphoreType.DMA
NX, NZ, NY = 4, 8, 4
CHUNKS, WIDE, LAG, PIECES = 8, 512, 4, 24


def place(x, z, y, s):
    return ((x * NZ + z) * NY + y, s)


def remote(src, dst, send, recv, device):
    return pltpu.make_async_remote_copy(
        src_ref=src, dst_ref=dst, send_sem=send, recv_sem=recv, device_id=device, device_id_type=MESH
    )


def each(lo, hi, body):
    lax.fori_loop(lo, hi, lambda i, c: (body(i), c)[1], 0)


def factor128(block, midway=None):
    lane = lax.broadcasted_iota(jnp.int32, (8, 128), 1)
    sub = lax.broadcasted_iota(jnp.int32, (8, 128), 0)
    below = block.reshape(16, 8, 128)
    uppers, inverses = [], []
    for p in range(16):
        if p == 3 and midway is not None:
            midway()
        n, first = 16 - p, 8 * p
        cols = [jnp.broadcast_to(below[:, :, first + j : first + j + 1], (n, 8, 128)) for j in range(8)]
        inside = (lane >= first) & (lane < first + 8)
        here = jnp.where(inside, (lane - first == sub).astype(F), below[0])[None]
        if n > 1:
            below = jnp.concatenate([here, jnp.where(inside[None], 0.0, below[1:])], axis=0)
        else:
            below = here
        pivot = jnp.ones((8, 128), F)
        for k in range(8):
            d = jnp.broadcast_to(cols[k][0, k : k + 1, :], (8, 128))
            pivot = jnp.where(sub == k, d, pivot)
            m = cols[k] * (1.0 / d)[None]
            top = jnp.where(sub > k, m[0], 0.0)[None]
            m = jnp.concatenate([top, m[1:]], axis=0) if n > 1 else top
            row = jnp.broadcast_to(below[0, k : k + 1, :], (8, 128))
            for j in range(k + 1, 8):
                u = jnp.broadcast_to(cols[j][0, k : k + 1, :], (8, 128))
                cols[j] = cols[j] - m * u[None]
            below = below - m * row[None]
        upper = jnp.where(lane < first + 8, 0.0, below[0])
        for j in range(8):
            upper = jnp.where((lane == first + j) & (sub <= j), cols[j][0], upper)
        scale = lax.rsqrt(pivot)
        uppers.append(scale * upper)
        inverses.append(scale * jnp.where(lane < first + 8, below[0], 0.0))
        below = below[1:]
    return jnp.concatenate(uppers, axis=0), jnp.concatenate(inverses, axis=0)


def times(a, b, turn=False):
    return lax.dot_general(a, b, (((0 if turn else 1,), (0,)), ((), ())), precision=HI, preferred_element_type=F)


def factor_first(t_ref, upper, inverse, midway=None):
    top, bottom = slice(0, 128), slice(128, 256)
    u, inv = factor128(t_ref[top, top], midway)
    side = times(inv, t_ref[top, bottom])
    t_ref[bottom, bottom] = t_ref[bottom, bottom] - times(side, side, True)
    upper[top, top] = u
    upper[top, bottom] = side
    inverse[top, top] = inv
    inverse[top, bottom] = jnp.zeros((128, 128), F)


def factor_last(t_ref, upper, inverse):
    top, bottom = slice(0, 128), slice(128, 256)
    u, inv = factor128(t_ref[bottom, bottom])
    upper[bottom, bottom] = u
    upper[bottom, top] = jnp.zeros((128, 128), F)
    inverse[bottom, bottom] = inv
    inverse[bottom, top] = -times(inv, times(upper[top, bottom], inverse[top, top], True))


def reduce_kernel(
    movie, test, pair, upper, inverse, cross,
    mv, tv, sketch, turned, grown, part, drecv, half, gpart, grs, gz, gram, t_ref,
    a_tmp, a_in, b_tmp, b_in, pa, pb, r2, p2, r3, p3,
    msem, tsem, dsend, drsem, gs_send, gs_recv, gz_send, gz_recv, ga_send, ga_recv,
    s1_send, s1_recv, s2_send, s2_recv, s3_send, s3_recv, s4_send, s4_recv,
):
    vox, s = lax.axis_index("vox"), lax.axis_index("sub")
    y = lax.rem(vox, NY)
    z = lax.rem(lax.div(vox, NY), NZ)
    x = lax.div(vox, NY * NZ)
    q = (x * NY + y) * 2 + s
    other = place(x, z, y, 1 - s)

    def load(c):
        wide = pl.ds(pl.multiple_of(c * WIDE, WIDE), WIDE)
        return (
            pltpu.make_async_copy(movie.at[:, wide], mv.at[c], msem.at[c]),
            pltpu.make_async_copy(test.at[wide], tv.at[c], tsem.at[c]),
        )

    def start(c):
        for copy in load(c):
            copy.start()

    each(0, CHUNKS, start)

    def plane(d):
        t = lax.rem(q + d, 32)
        return t, place(lax.div(t, NY * 2), z, lax.rem(lax.div(t, 2), NY), lax.rem(t, 2))

    def column(d):
        t = lax.rem(z + d, NZ)
        return t, place(x, t, y, s)

    barrier = pltpu.get_barrier_semaphore()

    def greet(device):
        pl.semaphore_signal(barrier, inc=1, device_id=device, device_id_type=MESH)

    each(1, 32, lambda d: greet(plane(d)[1]))
    each(1, NZ, lambda d: greet(column(d)[1]))

    sketch[...] = jnp.zeros_like(sketch)

    def project(c):
        for copy in load(c):
            copy.wait()
        sketch[...] += jnp.dot(mv[c], tv[c], preferred_element_type=F)

    each(0, CHUNKS, project)
    near = sketch[...].astype(jnp.bfloat16)
    pair[...] = jnp.concatenate([near, (sketch[...] - near.astype(F)).astype(jnp.bfloat16)], axis=1)
    turned[...] = jnp.transpose(pair[...])
    grown[...] = jnp.dot(turned[...], pair[...], preferred_element_type=F)
    low, high = slice(0, 256), slice(256, 512)
    product = (grown[low, low] + grown[high, high]) + (grown[low, high] + grown[high, low])
    top, bottom = slice(0, 128), slice(128, 256)
    quarters = ((top, top), (top, bottom), (bottom, bottom))
    for i, (a, b) in enumerate(quarters):
        gpart[8 * i : 8 * i + 8] = product[a, b].reshape(8, 16, 128)

    xr, xo, xl = (lax.rem(x + d, NX) for d in (1, 2, 3))
    yr, yo, yl = (lax.rem(y + d, NY) for d in (1, 2, 3))
    right_x, left_x = place(xr, z, y, s), place(xl, z, y, s)
    right_y, left_y = place(x, z, yr, s), place(x, z, yl, s)

    turn = lax.rem(x + y, 4)
    owner = turn < 3
    mine = (x * 3 + lax.min(turn, 2)) * 2 + s

    def others(body):
        def visit(j):
            t = lax.rem(mine + j, PIECES)
            tx, ts = lax.div(t, 6), lax.rem(t, 2)
            ty = lax.rem(lax.rem(lax.div(t, 2), 3) - tx + 4, 4)
            at = (tx * NY + ty) * 2 + ts

            @pl.when(at != q)
            def _():
                body(t, at, place(tx, z, ty, ts))

        each(0, PIECES, visit)

    pl.semaphore_wait(barrier, 31 + NZ - 1)

    def gram_scatter(t, at, device):
        d = lax.rem(at - q + 32, 32)
        return remote(gpart.at[t], grs.at[d], gs_send.at[t], gs_recv.at[d], device)

    others(lambda *a: gram_scatter(*a).start())

    def across(i):
        rows = pl.ds(pl.multiple_of((1 - s) * 128, 128), 128)
        return remote(part.at[i, rows], drecv.at[i], dsend.at[i], drsem.at[i], other)

    def multiply(i):
        h, r = i // 4, i % 4
        chunk = 2 * lax.rem(xo + r, NX) + h
        part[i] = jnp.dot(turned[low], mv[chunk], preferred_element_type=F)
        across(i).start()

    be, af, every = pl.ds(0, 2), pl.ds(2, 2), pl.ds(0, 4)

    def ring(h, i, src, dst, device):
        return remote(src, dst, s1_send.at[h, i], s1_recv.at[h, i], device)

    ring_a = [
        [
            ring(h, 0, half.at[h, 0, be], a_tmp.at[h, 0], right_x),
            ring(h, 1, half.at[h, 0, af], a_tmp.at[h, 1], left_x),
            ring(h, 2, half.at[h, 3, af], a_in.at[h, 0, af], right_x),
            ring(h, 3, half.at[h, 1, be], a_in.at[h, 1, be], left_x),
            ring(h, 4, half.at[h, 3, be], a_in.at[h, 0, be], right_x),
            ring(h, 5, half.at[h, 1, af], a_in.at[h, 1, af], left_x),
        ]
        for h in range(2)
    ]
    ring_b = [
        [
            ring(h, 0, half.at[h, be, every, yo], b_tmp.at[h, 0], right_y),
            ring(h, 1, half.at[h, af, every, yo], b_tmp.at[h, 1], left_y),
            ring(h, 2, half.at[h, af, every, yr], b_in.at[h, 0, af], right_y),
            ring(h, 3, half.at[h, be, every, yl], b_in.at[h, 1, be], left_y),
            ring(h, 4, half.at[h, be, every, yr], b_in.at[h, 0, be], right_y),
            ring(h, 5, half.at[h, af, every, yl], b_in.at[h, 1, af], left_y),
        ]
        for h in range(2)
    ]

    def begin(h, a, b):
        @pl.when(s == 0)
        def _():
            for i in a:
                ring_a[h][i].start()

        @pl.when(s == 1)
        def _():
            for i in b:
                ring_b[h][i].start()

    after = {0: ((0, 1), ()), 1: ((3,), (0, 3)), 3: ((2,), (1, 2))}
    for step in range(CHUNKS + LAG):
        if step < CHUNKS:
            multiply(step)
        i = step - LAG
        if i >= 0:
            across(i).wait_recv()
            both = part[i, pl.ds(pl.multiple_of(s * 128, 128), 128)] + drecv[i]
            half[i // 4, i % 4] = jnp.transpose(both).reshape(4, NY, 32, 128)
            if i % 4 in after:
                begin(i // 4, *after[i % 4])

    def ring_again(h):
        @pl.when(s == 0)
        def _():
            ring_a[h][0].wait_recv()
            half[h, 3, be] = half[h, 3, be] + a_tmp[h, 0]
            ring_a[h][4].start()
            ring_a[h][1].wait_recv()
            half[h, 1, af] = half[h, 1, af] + a_tmp[h, 1]
            ring_a[h][5].start()

        @pl.when(s == 1)
        def _():
            ring_b[h][0].wait_recv()
            half[h, be, every, yr] = half[h, be, every, yr] + b_tmp[h, 0]
            ring_b[h][4].start()
            ring_b[h][1].wait_recv()
            half[h, af, every, yl] = half[h, af, every, yl] + b_tmp[h, 1]
            ring_b[h][5].start()

    def second_a(h, d):
        t = (yr, yo, yl)[d]
        return remote(pa.at[h, every, t], r2.at[h, d], s2_send.at[h, d], s2_recv.at[h, d], place(x, z, t, s))

    def second_b(h, d):
        t = (xr, xo, xl)[d]
        return remote(pb.at[h, (3, 0, 1)[d]], r2.at[h, d], s2_send.at[h, d], s2_recv.at[h, d], place(t, z, y, s))

    def second(h):
        @pl.when(s == 0)
        def _():
            for copy in ring_a[h][2:]:
                copy.wait_recv()
            pa[h] = half[h, 2] + a_in[h, 0] + a_in[h, 1]
            for d in range(3):
                second_a(h, d).start()

        @pl.when(s == 1)
        def _():
            for copy in ring_b[h][2:]:
                copy.wait_recv()
            pb[h] = half[h, :, :, y] + b_in[h, 0] + b_in[h, 1]
            for d in range(3):
                second_b(h, d).start()

    def third(d):
        t, device = column(d)
        return remote(p2.at[t], r3.at[d], s3_send.at[d], s3_recv.at[d], device)

    def third_start(h):
        for d in range(3):
            second_a(h, d).wait_recv()

        @pl.when(s == 0)
        def _():
            p2[4 * h : 4 * h + 4] = pa[h, :, y] + r2[h, 0] + r2[h, 1] + r2[h, 2]

        @pl.when(s == 1)
        def _():
            p2[4 * h : 4 * h + 4] = pb[h, 2] + r2[h, 0] + r2[h, 1] + r2[h, 2]

        def visit(d):
            @pl.when(lax.div(column(d)[0], 4) == h)
            def _():
                third(d).start()

        each(1, NZ, visit)

    def gram_column(d):
        t, device = column(d)
        return remote(gz.at[z], gz.at[z], gz_send.at[d], gz_recv.at[d], device)

    def gram_column_from(d):
        t = lax.rem(z - d + NZ, NZ)
        return remote(gz.at[t], gz.at[t], gz_send.at[d], gz_recv.at[d], place(x, t, y, s))

    def gram_gather(d):
        return remote(gram.at[mine], gram.at[mine], ga_send.at[d], ga_recv.at[mine], plane(d)[1])

    def gram_gather_from(t, at, device):
        return remote(gram.at[t], gram.at[t], ga_send.at[0], ga_recv.at[t], device)

    def gram_pieces():
        @pl.when(owner)
        def _():
            each(1, 32, lambda d: remote(gpart.at[0], grs.at[d], gs_send.at[0], gs_recv.at[d], other).wait_recv())
            total = gpart[mine]
            for d in range(1, 32):
                total = total + grs[d]
            gz[z] = total
            each(1, NZ, lambda d: gram_column(d).start())

    def gram_totals():
        @pl.when(owner)
        def _():
            each(1, NZ, lambda d: gram_column_from(d).wait_recv())
            each(1, NZ, lambda d: gram_column(d).wait_send())
            total = gz[0]
            for j in range(1, NZ):
                total = total + gz[j]
            gram[mine] = total
            each(1, 32, lambda d: gram_gather(d).start())

    def gram_whole():
        others(lambda *a: gram_gather_from(*a).wait_recv())
        for i, (a, b) in enumerate(quarters):
            t_ref[a, b] = gram[8 * i : 8 * i + 8].reshape(128, 128)

    gram_pieces()
    ring_again(0)
    ring_again(1)
    gram_totals()
    second(0)
    second(1)
    third_start(0)
    gram_whole()
    factor_first(t_ref, upper, inverse, lambda: third_start(1))
    factor_last(t_ref, upper, inverse)

    each(1, NZ, lambda d: third(d).wait_recv())
    total = p2[z]
    for d in range(1, NZ):
        total = total + r3[d]
    p3[...] = total.reshape(2, 16, 128)
    last = remote(p3.at[1 - s], cross.at[s], s4_send.at[0], s4_recv.at[0], other)
    last.start()
    cross[s] = p3[s]
    remote(p3.at[s], cross.at[1 - s], s4_send.at[0], s4_recv.at[0], other).wait_recv()

    others(lambda *a: gram_scatter(*a).wait_send())

    @pl.when(owner)
    def _():
        each(1, 32, lambda d: gram_gather(d).wait_send())

    each(0, CHUNKS, lambda i: across(i).wait_send())
    each(1, NZ, lambda d: third(d).wait_send())
    last.wait_send()

    @pl.when(s == 0)
    def _():
        for h in range(2):
            for copy in ring_a[h]:
                copy.wait_send()
            for d in range(3):
                second_a(h, d).wait_send()

    @pl.when(s == 1)
    def _():
        for h in range(2):
            for copy in ring_b[h]:
                copy.wait_send()
            for d in range(3):
                second_b(h, d).wait_send()


def finish_kernel(voxels, pair, upper, inverse, cross, basis, r_factor, projected):
    scale = jnp.sqrt(F(voxels))
    turned = jnp.transpose(inverse[...])
    scaled = turned * scale
    near = scaled.astype(jnp.bfloat16)
    rest = (scaled - near.astype(F)).astype(jnp.bfloat16)
    basis[...] = jnp.dot(pair[...], jnp.concatenate([near, near], axis=0), preferred_element_type=F) + jnp.dot(
        pair[:, :256], rest, preferred_element_type=F
    )
    r_factor[...] = upper[...] / scale
    both = jnp.concatenate([cross[0], cross[1]], axis=1)
    projected[...] = jnp.dot(both, turned, precision=HI, preferred_element_type=F)


def local(movie, test_matrix):
    shape = jax.ShapeDtypeStruct
    movie, test_matrix = (pltpu.with_memory_space_constraint(a, pltpu.HBM) for a in (movie, test_matrix))
    in_vmem = pl.BlockSpec(memory_space=VMEM)
    square = shape((256, 256), F)
    pair, upper, inverse, cross = pl.pallas_call(
        reduce_kernel,
        out_shape=(shape((1024, 512), jnp.bfloat16), square, square, shape((2, 16, 128), F)),
        in_specs=[pl.BlockSpec(memory_space=pltpu.HBM)] * 2,
        out_specs=[in_vmem] * 4,
        scratch_shapes=[
            VMEM((CHUNKS, 1024, WIDE), jnp.bfloat16),
            VMEM((CHUNKS, WIDE, 256), jnp.bfloat16),
            VMEM((1024, 256), F),
            VMEM((512, 1024), jnp.bfloat16),
            VMEM((512, 512), F),
            VMEM((CHUNKS, 256, WIDE), F),
            VMEM((CHUNKS, 128, WIDE), F),
            VMEM((2, NX, 4, NY, 32, 128), F),
            VMEM((PIECES, 16, 128), F),
            VMEM((32, 16, 128), F),
            VMEM((NZ, 16, 128), F),
            VMEM((PIECES, 16, 128), F),
            VMEM((256, 256), F),
            VMEM((2, 2, 2, NY, 32, 128), F),
            VMEM((2, 2, 4, NY, 32, 128), F),
            VMEM((2, 2, 2, 4, 32, 128), F),
            VMEM((2, 2, NX, 4, 32, 128), F),
            VMEM((2, 4, NY, 32, 128), F),
            VMEM((2, NX, 4, 32, 128), F),
            VMEM((2, 3, 4, 32, 128), F),
            VMEM((NZ, 32, 128), F),
            VMEM((NZ, 32, 128), F),
            VMEM((2, 16, 128), F),
        ]
        + [DMA((n,)) for n in (8, 8, 8, 8, PIECES, 32, 8, 8, 32, PIECES)]
        + [DMA(n) for n in ((2, 6), (2, 6), (2, 3), (2, 3), (8,), (8,), (1,), (1,))],
        compiler_params=pltpu.CompilerParams(
            collective_id=0, has_side_effects=True, vmem_limit_bytes=40 * 1024 * 1024
        ),
    )(movie, test_matrix)
    voxels = movie.shape[0] * NX * NY * NZ * 2
    basis, r_factor, projected = pl.pallas_call(
        lambda *refs: finish_kernel(voxels, *refs),
        out_shape=(shape((1024, 256), F), square, shape((16, 256), F)),
        in_specs=[in_vmem] * 4,
        out_specs=[in_vmem] * 3,
        compiler_params=pltpu.CompilerParams(vmem_limit_bytes=16 * 1024 * 1024),
    )(pair, upper, inverse, cross)
    return basis, r_factor, projected.T


def solution(mesh):
    placed = (P(("vox", "sub"), None), P())
    return jax.shard_map(
        local,
        mesh=mesh,
        in_specs=placed,
        out_specs=(P(("vox", "sub"), None), P(), P(None, ("vox", "sub"))),
        check_vma=False,
    )
```
